32 devices in a mesh: shard: 4 (over z), width: 2 (over core), shift: 4 (over y, x).
Axes of the slice: x: 2, y: 2, z: 4, core: 2. Of those that a mesh axis runs over, the one named last changes fastest.
Arguments:
- w_query: bfloat16 [8192, 2048], P(('shift', 'shard'), 'width'), parts along dimension 0, may hold values from -0.125 to 0.125
- low_query: bfloat16 [8192, 16], P(('shift', 'shard')), parts along dimension 0, may hold values from -0.125 to 0.125
- high_query: bfloat16 [64, 2048], P('shift', 'width'), parts along dimension 0, may hold values from -1.5 to 1.5
- w_key: bfloat16 [8192, 512], P(('shift', 'shard'), 'width'), parts along dimension 0, may hold values from -0.125 to 0.125
- low_key: bfloat16 [8192, 16], P(('shift', 'shard')), parts along dimension 0, may hold values from -0.125 to 0.125
- high_key: bfloat16 [64, 512], P('shift', 'width'), parts along dimension 0, may hold values from -1.5 to 1.5
- w_value: bfloat16 [8192, 512], P(('shift', 'shard'), 'width'), parts along dimension 0, may hold values from -0.125 to 0.125
- low_value: bfloat16 [8192, 16], P(('shift', 'shard')), parts along dimension 0, may hold values from -0.125 to 0.125
- high_value: bfloat16 [64, 512], P('shift', 'width'), parts along dimension 0, may hold values from -1.5 to 1.5
- w_mixed: bfloat16 [8192, 2048], P(('shift', 'width'), 'shard'), parts along dimension 0, may hold values from -0.125 to 0.125
- low_mixed: bfloat16 [8192, 16], P(('shift', 'width')), parts along dimension 0, may hold values from -0.125 to 0.125
- high_mixed: bfloat16 [64, 2048], P('shift', 'shard'), parts along dimension 0, may hold values from -1.5 to 1.5
- norm_train: float32 [8192], P(('shift', 'shard', 'width')), parts along dimension 0, may hold values from 0.25 to 1.75
- norm_step: float32 [8192], P(('shift', 'shard', 'width')), parts along dimension 0, may hold values from -0.3 to 0.3
Outputs:
- final_query: bfloat16 [8192, 2048], P(('shift', 'width')), parts along dimension 0
- final_key: bfloat16 [2048, 2048], P(('shift', 'width')), parts along dimension 0
- final_value: bfloat16 [2048, 2048], P(('shift', 'width')), parts along dimension 0
- final_mixed: bfloat16 [8192, 2048], P('shift', 'width'), parts along dimension 0
- serve_norm: bfloat16 [8192], P('shift'), parts along dimension 0
The draws below stay inside these ranges and needn't reach their ends.
There are 4 independent parts, one for each index of `shift`. The reference program is written for one: setup_inputs(seed, part) draws one part's arguments, and reference() takes and returns one part's arrays. A program takes and returns all parts, laid end to end along the dimension named above; each array names one. Nothing has to cross between parts.
All inputs are finite; a program needn't handle non-finite values.
Results may differ from the reference program's by a relative error of at most 0.001.
Values may be sent and summed in bfloat16 or wider, within the bound.
A program may use at most 64 MiB of HBM per device.

```python
import jax
import jax.numpy as jnp

D_MODEL = 2048
Q_DIM = 2048
KV_DIM = 512
RANK = 16


def levels(key, shape, pieces, low, top_value):
    gain, own = 1.0, jax.random.fold_in(key, 6)
    for dim, shards_of in pieces:
        heights = jnp.exp(jax.random.uniform(jax.random.fold_in(own, dim), (shards_of,), jnp.float32, low / len(pieces), top_value / len(pieces)))
        gain = gain * jnp.repeat(heights, shape[dim] // shards_of).reshape([-1 if axis == dim else 1 for axis in range(len(shape))])
    return gain


def noise(own_key, shape, width, bound, shards=(), dtype=jnp.bfloat16):
    array = width * jax.random.normal(own_key, shape, jnp.float32)
    if shards:
        array = array * levels(own_key, shape, shards, -0.22, 0.18)
    return jnp.clip(array, -bound, bound).astype(dtype)


def setup_inputs(seed: int = 0, part: int = 0) -> dict:
    keys = jax.random.split(jax.random.key(seed), 15)
    own_keys = jax.random.split(jax.random.fold_in(keys[14], part), 15)
    w_query = noise(own_keys[0], (D_MODEL, Q_DIM), D_MODEL ** -0.5, 0.125, ((0, 4), (1, 2)))
    low_query = noise(own_keys[1], (D_MODEL, RANK), D_MODEL ** -0.5, 0.125, ((0, 4),))
    high_query = noise(own_keys[2], (RANK, Q_DIM), RANK ** -0.5, 1.5, ((1, 2),))
    w_key = noise(own_keys[3], (D_MODEL, KV_DIM), D_MODEL ** -0.5, 0.125, ((0, 4), (1, 2)))
    low_key = noise(own_keys[4], (D_MODEL, RANK), D_MODEL ** -0.5, 0.125, ((0, 4),))
    high_key = noise(own_keys[5], (RANK, KV_DIM), RANK ** -0.5, 1.5, ((1, 2),))
    w_value = noise(own_keys[6], (D_MODEL, KV_DIM), D_MODEL ** -0.5, 0.125, ((0, 4), (1, 2)))
    low_value = noise(own_keys[7], (D_MODEL, RANK), D_MODEL ** -0.5, 0.125, ((0, 4),))
    high_value = noise(own_keys[8], (RANK, KV_DIM), RANK ** -0.5, 1.5, ((1, 2),))
    w_mixed = noise(own_keys[9], (Q_DIM, D_MODEL), Q_DIM ** -0.5, 0.125, ((0, 2), (1, 4)))
    low_mixed = noise(own_keys[10], (Q_DIM, RANK), Q_DIM ** -0.5, 0.125, ((0, 2),))
    high_mixed = noise(own_keys[11], (RANK, D_MODEL), RANK ** -0.5, 1.5, ((1, 4),))
    norm_train = jnp.clip(1.0 + 0.15 * jax.random.normal(own_keys[12], (D_MODEL,), jnp.float32), 0.25, 1.75)
    norm_step = jnp.clip(jax.random.uniform(own_keys[13], (D_MODEL,), jnp.float32, -0.3, 0.3) * levels(own_keys[13], (D_MODEL,), ((0, 8),), -0.4, 0.0), -0.3, 0.3)
    return dict(w_query=w_query, low_query=low_query, high_query=high_query, w_key=w_key, low_key=low_key, high_key=high_key, w_value=w_value, low_value=low_value, high_value=high_value, w_mixed=w_mixed, low_mixed=low_mixed, high_mixed=high_mixed, norm_train=norm_train, norm_step=norm_step)


mix_rate = 0.5


def reference(w_query, low_query, high_query, w_key, low_key, high_key, w_value, low_value, high_value, w_mixed, low_mixed, high_mixed, norm_train, norm_step):
    result_query = w_query.astype(jnp.float32) + mix_rate * jnp.dot(low_query, high_query, preferred_element_type=jnp.float32)
    result_key = w_key.astype(jnp.float32) + mix_rate * jnp.dot(low_key, high_key, preferred_element_type=jnp.float32)
    result_value = w_value.astype(jnp.float32) + mix_rate * jnp.dot(low_value, high_value, preferred_element_type=jnp.float32)
    result_mixed = w_mixed.astype(jnp.float32) + mix_rate * jnp.dot(low_mixed, high_mixed, preferred_element_type=jnp.float32)
    final_query = result_query.T.astype(jnp.bfloat16)
    final_key = result_key.T.astype(jnp.bfloat16)
    final_value = result_value.T.astype(jnp.bfloat16)
    final_mixed = result_mixed.T.astype(jnp.bfloat16)
    serve_norm = (norm_train + norm_step).astype(jnp.bfloat16)
    return final_query, final_key, final_value, final_mixed, serve_norm
```

```python
import functools

import jax
import jax.numpy as jnp
from jax import lax
from jax.experimental import pallas as pl
from jax.experimental.pallas import tpu as pltpu
from jax.sharding import PartitionSpec as P

mix_rate = 0.5
MESH = pl.DeviceIdType.MESH
LANES = 128
SUBLANES = 8


def plain(
    w_query,
    low_query,
    high_query,
    w_key,
    low_key,
    high_key,
    w_value,
    low_value,
    high_value,
    w_mixed,
    low_mixed,
    high_mixed,
    norm_train,
    norm_step,
):
    def merged(w, low, high):
        low_rank = jnp.dot(low, high, preferred_element_type=jnp.float32)
        return (w.astype(jnp.float32) + mix_rate * low_rank).astype(jnp.bfloat16)

    query = lax.all_gather(merged(w_query, low_query, high_query), "shard", axis=0, tiled=True)
    key = lax.all_gather(merged(w_key, low_key, high_key), "shard", axis=0, tiled=True)
    value = lax.all_gather(merged(w_value, low_value, high_value), "shard", axis=0, tiled=True)
    mixed = lax.all_gather(merged(w_mixed, low_mixed, high_mixed), "shard", axis=1, tiled=True)
    norm = lax.all_gather(
        (norm_train + norm_step).astype(jnp.bfloat16), ("shard", "width"), axis=0, tiled=True
    )
    return query.T, key.T, value.T, mixed.T, norm


def kernel(
    n,
    given,
    train_ref,
    step_ref,
    outs,
    norm_out,
    copied,
    load_sem,
    send_sem,
    back_sem,
    recv_sem,
    pair_sem,
):
    me = lax.axis_index("shard")
    core = lax.axis_index("width")
    has_left, has_right = me > 0, me < n - 1
    left, right = {"shard": me - 1}, {"shard": me + 1}
    partner = {"width": 1 - core}

    loads = [
        pltpu.make_async_copy(source, copy, load_sem.at[i])
        for i, (source, copy) in enumerate(zip(given, copied))
    ]
    held, low_refs, high_refs = copied[0::3], copied[1::3], copied[2::3]
    for load in loads:
        load.start()

    barrier = pltpu.get_barrier_semaphore()
    pl.semaphore_signal(barrier, inc=1, device_id=partner, device_id_type=MESH)

    @pl.when(has_left)
    def _():
        pl.semaphore_signal(barrier, inc=1, device_id=left, device_id_type=MESH)

    @pl.when(has_right)
    def _():
        pl.semaphore_signal(barrier, inc=1, device_id=right, device_id_type=MESH)

    def piece(array, c, origin):
        if array == len(outs):
            return norm_out.at[origin]
        out, w = outs[array], held[array]
        if array < len(outs) - 1:
            block = w.shape[0]
            start = pl.multiple_of(origin * block, LANES)
            return out.at[pl.ds(pl.multiple_of(c * LANES, LANES), LANES), pl.ds(start, block)]
        start = pl.multiple_of(origin * w.shape[1] + c * LANES, LANES)
        return out.at[pl.ds(start, LANES)]

    counts = [w.shape[1] // LANES for w in held] + [1]
    firsts = [sum(counts[:i]) for i in range(len(counts))]

    def forward(array, c, origin):
        slot = firsts[array] + c
        return pltpu.make_async_remote_copy(
            src_ref=piece(array, c, origin),
            dst_ref=piece(array, c, origin),
            send_sem=send_sem.at[origin, slot],
            recv_sem=recv_sem.at[origin, slot],
            device_id=right,
            device_id_type=MESH,
        )

    def backward(array, c, origin, own=False):
        slot = firsts[array] + c
        return pltpu.make_async_remote_copy(
            src_ref=piece(array, c, origin),
            dst_ref=piece(array, c, origin),
            send_sem=back_sem.at[slot] if own else send_sem.at[origin, slot],
            recv_sem=recv_sem.at[origin, slot],
            device_id=left,
            device_id_type=MESH,
        )

    def compute(array, c):
        columns = pl.ds(pl.multiple_of(c * LANES, LANES), LANES)
        low_rank = lax.dot_general(
            high_refs[array][:, columns],
            low_refs[array][...],
            (((0,), (0,)), ((), ())),
            preferred_element_type=jnp.float32,
        )
        base = held[array][:, columns].astype(jnp.float32).T
        piece(array, c, me)[...] = (base + mix_rate * low_rank).astype(jnp.bfloat16)

    def send(array, c):
        @pl.when(has_right)
        def _():
            forward(array, c, me).start()

        @pl.when(has_left)
        def _():
            backward(array, c, me, own=True).start()

    norm_out[me, core] = train_ref[...] + step_ref[...]
    for load in loads[:3]:
        load.wait()
    compute(0, 0)

    pl.semaphore_wait(barrier, 1 + has_left.astype(jnp.int32) + has_right.astype(jnp.int32))

    pair = pltpu.make_async_remote_copy(
        src_ref=norm_out.at[me, core],
        dst_ref=norm_out.at[me, core],
        send_sem=pair_sem.at[0],
        recv_sem=pair_sem.at[1],
        device_id=partner,
        device_id_type=MESH,
    )
    pair.start()

    for array in range(len(outs)):
        if array:
            for load in loads[3 * array : 3 * array + 3]:
                load.wait()
            compute(array, 0)
            send(array - 1, counts[array - 1] - 1)

        def step(c, carry, array=array):
            compute(array, c)
            send(array, c - 1)
            return carry

        lax.fori_loop(1, counts[array], step, 0)
    pair.wait_send()
    pltpu.make_async_remote_copy(
        src_ref=norm_out.at[me, 1 - core],
        dst_ref=norm_out.at[me, 1 - core],
        send_sem=pair_sem.at[0],
        recv_sem=pair_sem.at[1],
        device_id=partner,
        device_id_type=MESH,
    ).wait_recv()
    send(len(outs) - 1, counts[len(outs) - 1] - 1)
    send(len(outs), 0)

    for k in range(1, n):
        from_left, from_right = me - k, me + k
        for array in range(len(counts)):

            def relay(c, carry, array=array, from_left=from_left, from_right=from_right):
                @pl.when(from_left >= 0)
                def _():
                    forward(array, c, from_left).wait_recv()

                    @pl.when(has_right)
                    def _():
                        forward(array, c, from_left).start()

                @pl.when(from_right < n)
                def _():
                    backward(array, c, from_right).wait_recv()

                    @pl.when(has_left)
                    def _():
                        backward(array, c, from_right).start()

                return carry

            lax.fori_loop(0, counts[array], relay, 0)

    for array in range(len(counts)):

        def drain(c, carry, array=array):
            @pl.when(has_right)
            def _():
                forward(array, c, me).wait_send()

            @pl.when(has_left)
            def _():
                backward(array, c, me, own=True).wait_send()

            for k in range(1, n):

                @pl.when(jnp.logical_and(me - k >= 0, has_right))
                def _(k=k):
                    forward(array, c, me - k).wait_send()

                @pl.when(jnp.logical_and(me + k < n, has_left))
                def _(k=k):
                    backward(array, c, me + k).wait_send()

            return carry

        lax.fori_loop(0, counts[array], drain, 0)


def body(n, *refs):
    kernel(n, refs[:12], refs[12], refs[13], refs[14:18], refs[18], refs[19:31], *refs[31:])


def on_device(n, cores, *args):
    weights, (norm_train, norm_step) = list(args[:12]), args[12:]
    bases = weights[0::3]
    whole_tiles = cores == 2 and all(size % LANES == 0 for w in bases for size in w.shape)
    if not whole_tiles:
        return plain(*args)
    (size,) = norm_train.shape
    tile = SUBLANES * LANES
    rows = -(-size // tile) * SUBLANES
    padding = rows * LANES - size

    def tiled(norm):
        return jnp.pad(norm, (0, padding)).reshape(rows, LANES)

    shapes = [(w.shape[1], w.shape[0] * n) for w in bases[:3]]
    shapes.append((bases[3].shape[1] * n, bases[3].shape[0]))
    slots = sum(w.shape[1] // LANES for w in bases) + 1
    weights[1::3] = [low.T for low in weights[1::3]]
    weights = [pltpu.with_memory_space_constraint(w, pltpu.HBM) for w in weights]
    in_hbm = pl.BlockSpec(memory_space=pltpu.HBM)
    in_vmem = pl.BlockSpec(memory_space=pltpu.VMEM)
    *finals, norm = pl.pallas_call(
        functools.partial(body, n),
        out_shape=[pltpu.VMEM(shape, jnp.bfloat16) for shape in shapes]
        + [pltpu.VMEM((n, cores, rows, LANES), jnp.float32)],
        in_specs=[in_hbm] * 12 + [in_vmem] * 2,
        out_specs=[in_vmem] * 5,
        scratch_shapes=[pltpu.VMEM(w.shape, w.dtype) for w in weights]
        + [
            pltpu.SemaphoreType.DMA((12,)),
            pltpu.SemaphoreType.DMA((n, slots)),
            pltpu.SemaphoreType.DMA((slots,)),
            pltpu.SemaphoreType.DMA((n, slots)),
            pltpu.SemaphoreType.DMA((2,)),
        ],
        compiler_params=pltpu.CompilerParams(
            collective_id=0, has_side_effects=True, vmem_limit_bytes=40 * 2**20
        ),
        name="merge_gather",
    )(*weights, tiled(norm_train), tiled(norm_step))
    serve_norm = norm.reshape(n * cores, rows * LANES)[:, :size].reshape(-1).astype(jnp.bfloat16)
    return (*finals, serve_norm)


def solution(mesh):
    placed = (
        P(("shift", "shard"), "width"),
        P(("shift", "shard"), None),
        P("shift", "width"),
        P(("shift", "shard"), "width"),
        P(("shift", "shard"), None),
        P("shift", "width"),
        P(("shift", "shard"), "width"),
        P(("shift", "shard"), None),
        P("shift", "width"),
        P(("shift", "width"), "shard"),
        P(("shift", "width"), None),
        P("shift", "shard"),
        P(("shift", "shard", "width")),
        P(("shift", "shard", "width")),
    )
    return jax.shard_map(
        functools.partial(on_device, mesh.shape["shard"], mesh.shape["width"]),
        mesh=mesh,
        in_specs=placed,
        out_specs=(
            P(("shift", "width"), None),
            P(("shift", "width"), None),
            P(("shift", "width"), None),
            P("shift", "width"),
            P("shift"),
        ),
        check_vma=False,
    )
```

```python
import functools

import jax
import jax.numpy as jnp
from jax import lax
from jax.experimental import pallas as pl
from jax.experimental.pallas import tpu as pltpu
from jax.sharding import PartitionSpec as P

mix_rate = 0.5
MESH = pl.DeviceIdType.MESH
LANES = 128
COPY_ROWS = 256
LATE_STEPS = 8
LATE_PIECES = 2


def plain(
    w_query,
    low_query,
    high_query,
    w_key,
    low_key,
    high_key,
    w_value,
    low_value,
    high_value,
    w_mixed,
    low_mixed,
    high_mixed,
    norm_train,
    norm_step,
):
    def merged(w, low, high):
        low_rank = jnp.dot(low, high, preferred_element_type=jnp.float32)
        return (w.astype(jnp.float32) + mix_rate * low_rank).astype(jnp.bfloat16)

    query = lax.all_gather(merged(w_query, low_query, high_query), "shard", axis=0, tiled=True)
    key = lax.all_gather(merged(w_key, low_key, high_key), "shard", axis=0, tiled=True)
    value = lax.all_gather(merged(w_value, low_value, high_value), "shard", axis=0, tiled=True)
    mixed = lax.all_gather(merged(w_mixed, low_mixed, high_mixed), "shard", axis=1, tiled=True)
    norm = lax.all_gather(
        (norm_train + norm_step).astype(jnp.bfloat16), ("shard", "width"), axis=0, tiled=True
    )
    return query.T, key.T, value.T, mixed.T, norm


def late_pieces(block):
    return min(LATE_PIECES, block // LANES)


def kernel(
    n,
    given,
    outs,
    norm_out,
    copied,
    load_sem,
    send_sem,
    back_sem,
    recv_sem,
    pair_sem,
):
    me = lax.axis_index("shard")
    core = lax.axis_index("width")
    has_left, has_right = me > 0, me < n - 1
    left, right = {"shard": me - 1}, {"shard": me + 1}
    partner = {"width": 1 - core}

    held, low_refs, high_refs = copied[0:12:3], copied[1:12:3], copied[2:12:3]
    width = held[0].shape[1]
    first, rest = pl.ds(0, LANES), pl.ds(LANES, width - LANES)
    loads = [pltpu.make_async_copy(given[0].at[:, first], held[0].at[:, first], load_sem.at[0])]
    loads += [
        pltpu.make_async_copy(given[i], copied[i], load_sem.at[i]) for i in range(1, len(given))
    ]
    others = []
    if width > LANES:
        others.append(
            pltpu.make_async_copy(
                given[0].at[:, rest], held[0].at[:, rest], load_sem.at[len(loads)]
            )
        )
    for load in loads[:3] + others + loads[3:]:
        load.start()

    barrier = pltpu.get_barrier_semaphore()
    pl.semaphore_signal(barrier, inc=1, device_id=partner, device_id_type=MESH)

    @pl.when(has_left)
    def _():
        pl.semaphore_signal(barrier, inc=1, device_id=left, device_id_type=MESH)

    @pl.when(has_right)
    def _():
        pl.semaphore_signal(barrier, inc=1, device_id=right, device_id_type=MESH)

    def piece(array, c, origin):
        if array == len(outs):
            return norm_out.at[origin]
        out, w = outs[array], held[array]
        if array < len(outs) - 1:
            block = w.shape[0]
            start = pl.multiple_of(origin * block, LANES)
            return out.at[pl.ds(pl.multiple_of(c * LANES, LANES), LANES), pl.ds(start, block)]
        start = pl.multiple_of(origin * w.shape[1] + c * LANES, LANES)
        return out.at[pl.ds(start, LANES)]

    counts = [w.shape[1] // LANES for w in held] + [1]
    kept = counts[len(outs) - 1] - late_pieces(held[-1].shape[1])
    moved = list(counts)
    moved[len(outs) - 1] = jnp.where(core == 0, kept, counts[len(outs) - 1])
    firsts = [sum(counts[:i]) for i in range(len(counts))]

    def forward(array, c, origin):
        slot = firsts[array] + c
        return pltpu.make_async_remote_copy(
            src_ref=piece(array, c, origin),
            dst_ref=piece(array, c, origin),
            send_sem=send_sem.at[origin, slot],
            recv_sem=recv_sem.at[origin, slot],
            device_id=right,
            device_id_type=MESH,
        )

    def backward(array, c, origin, own=False):
        slot = firsts[array] + c
        return pltpu.make_async_remote_copy(
            src_ref=piece(array, c, origin),
            dst_ref=piece(array, c, origin),
            send_sem=back_sem.at[slot] if own else send_sem.at[origin, slot],
            recv_sem=recv_sem.at[origin, slot],
            device_id=left,
            device_id_type=MESH,
        )

    def compute(array, c):
        columns = pl.ds(pl.multiple_of(c * LANES, LANES), LANES)
        low_rank = lax.dot_general(
            high_refs[array][:, columns],
            low_refs[array][...],
            (((0,), (0,)), ((), ())),
            preferred_element_type=jnp.float32,
        )
        base = held[array][:, columns].astype(jnp.float32).T
        piece(array, c, me)[...] = (base + mix_rate * low_rank).astype(jnp.bfloat16)

    def send(array, c):
        ready = c < moved[array]

        @pl.when(jnp.logical_and(has_right, ready))
        def _():
            forward(array, c, me).start()

        @pl.when(jnp.logical_and(has_left, ready))
        def _():
            backward(array, c, me, own=True).start()

    for load in loads[:3]:
        load.wait()
    compute(0, 0)

    pl.semaphore_wait(barrier, 1 + has_left.astype(jnp.int32) + has_right.astype(jnp.int32))

    def exchange(side):
        return pltpu.make_async_remote_copy(
            src_ref=norm_out.at[me, side],
            dst_ref=norm_out.at[me, side],
            send_sem=pair_sem.at[0],
            recv_sem=pair_sem.at[1],
            device_id=partner,
            device_id_type=MESH,
        )

    for array in range(len(outs)):
        for load in loads[3 * array : 3 * array + 3] if array else others:
            load.wait()
        if array:
            compute(array, 0)
            send(array - 1, counts[array - 1] - 1)
        if array == 1:
            for load in loads[12:]:
                load.wait()
            norm_out[me, core] = copied[12][...] + copied[13][...]

        def step(c, carry, array=array):
            compute(array, c)
            send(array, c - 1)
            return carry

        lax.fori_loop(1, counts[array], step, 0)
    exchange(core).start()

    send(len(outs) - 1, counts[len(outs) - 1] - 1)

    exchange(core).wait_send()
    exchange(1 - core).wait_recv()
    send(len(outs), 0)

    for k in range(1, n):
        from_left, from_right = me - k, me + k
        for array in range(len(counts)):

            def relay(c, carry, array=array, from_left=from_left, from_right=from_right):
                @pl.when(from_left >= 0)
                def _():
                    forward(array, c, from_left).wait_recv()

                    @pl.when(has_right)
                    def _():
                        forward(array, c, from_left).start()

                @pl.when(from_right < n)
                def _():
                    backward(array, c, from_right).wait_recv()

                    @pl.when(has_left)
                    def _():
                        backward(array, c, from_right).start()

                return carry

            lax.fori_loop(0, moved[array], relay, 0)

    for array in range(len(counts)):

        def drain(c, carry, array=array):
            @pl.when(has_right)
            def _():
                forward(array, c, me).wait_send()

            @pl.when(has_left)
            def _():
                backward(array, c, me, own=True).wait_send()

            for k in range(1, n):

                @pl.when(jnp.logical_and(me - k >= 0, has_right))
                def _(k=k):
                    forward(array, c, me - k).wait_send()

                @pl.when(jnp.logical_and(me + k < n, has_left))
                def _(k=k):
                    backward(array, c, me + k).wait_send()

            return carry

        lax.fori_loop(0, moved[array], drain, 0)


def body(n, *refs):
    kernel(n, refs[:14], refs[14:18], refs[18], refs[19:33], *refs[33:])


def store(n, cores, *refs):
    gathered, norm_ref, outs, norm_out, flat, sem, mixed_sem = refs[:4], refs[4], refs[5:9], *refs[9:]
    me, core = lax.axis_index("shard"), lax.axis_index("width")
    copies = []
    for source, out in zip(gathered[:3], outs[:3]):
        for row in range(0, source.shape[0], COPY_ROWS):
            rows = pl.ds(row, min(COPY_ROWS, source.shape[0] - row))
            copies.append(
                pltpu.make_async_copy(source.at[rows], out.at[rows], sem.at[len(copies)])
            )

    block = gathered[3].shape[0] // n
    tail = late_pieces(block) * LANES

    def mixed(origin, row, size, part):
        rows = pl.ds(origin * block + row, size)
        return pltpu.make_async_copy(
            gathered[3].at[rows], outs[3].at[rows], mixed_sem.at[origin, part]
        )

    if block > tail:
        copies += [mixed(origin, 0, block - tail, 0) for origin in range(n)]

    def each_last(act):
        for origin in range(n):

            @pl.when(jnp.logical_or(core != 0, me == origin))
            def _(origin=origin):
                act(mixed(origin, block - tail, tail, 1))

    for copy in copies:
        copy.start()
    each_last(lambda copy: copy.start())
    rows = norm_ref.shape[2]
    for origin in range(n):
        for side in range(cores):
            flat[pl.ds((origin * cores + side) * rows, rows)] = norm_ref[origin, side]
    norm_out[...] = flat[...].astype(norm_out.dtype)
    for copy in copies:
        copy.wait()
    each_last(lambda copy: copy.wait())


def late(n, mixed, after, out, send_sem, back_sem, recv_sem):
    me = lax.axis_index("shard")
    core = lax.axis_index("width")
    has_left, has_right = me > 0, me < n - 1
    left, right = {"shard": me - 1}, {"shard": me + 1}
    block = mixed.shape[0] // n
    tail = late_pieces(block) * LANES
    size = tail // LATE_STEPS

    def copy(origin, step, device, semaphore, own):
        rows = pl.ds(pl.multiple_of(step * size, size), size)
        first = pl.multiple_of(me * block + block - tail + step * size, size)
        return pltpu.make_async_remote_copy(
            src_ref=mixed.at[pl.ds(first, size)] if own else out.at[origin, rows],
            dst_ref=out.at[origin, rows],
            send_sem=semaphore,
            recv_sem=recv_sem.at[origin, step],
            device_id=device,
            device_id_type=MESH,
        )

    def forward(origin, step, own=False):
        return copy(origin, step, right, send_sem.at[origin, step], own)

    def backward(origin, step, own=False):
        semaphore = back_sem.at[step] if own else send_sem.at[origin, step]
        return copy(origin, step, left, semaphore, own)

    @pl.when(core == 0)
    def _():
        barrier = pltpu.get_barrier_semaphore()

        @pl.when(has_left)
        def _():
            pl.semaphore_signal(barrier, inc=1, device_id=left, device_id_type=MESH)

        @pl.when(has_right)
        def _():
            pl.semaphore_signal(barrier, inc=1, device_id=right, device_id_type=MESH)

        pl.semaphore_wait(barrier, has_left.astype(jnp.int32) + has_right.astype(jnp.int32))

        for step in range(LATE_STEPS):

            @pl.when(has_right)
            def _(step=step):
                forward(me, step, own=True).start()

            @pl.when(has_left)
            def _(step=step):
                backward(me, step, own=True).start()

        for k in range(1, n):

            def relay(step, carry, k=k):
                @pl.when(me - k >= 0)
                def _():
                    forward(me - k, step).wait_recv()

                    @pl.when(has_right)
                    def _():
                        forward(me - k, step).start()

                @pl.when(me + k < n)
                def _():
                    backward(me + k, step).wait_recv()

                    @pl.when(has_left)
                    def _():
                        backward(me + k, step).start()

                return carry

            lax.fori_loop(0, LATE_STEPS, relay, 0)

        def drain(step, carry):
            @pl.when(has_right)
            def _():
                forward(me, step, own=True).wait_send()

            @pl.when(has_left)
            def _():
                backward(me, step, own=True).wait_send()

            for k in range(1, n):

                @pl.when(jnp.logical_and(me - k >= 0, has_right))
                def _(k=k):
                    forward(me - k, step).wait_send()

                @pl.when(jnp.logical_and(me + k < n, has_left))
                def _(k=k):
                    backward(me + k, step).wait_send()

            return carry

        lax.fori_loop(0, LATE_STEPS, drain, 0)


def store_late(n, pieces, given, out, sem):
    me, core = lax.axis_index("shard"), lax.axis_index("width")
    block = out.shape[0] // n
    tail = late_pieces(block) * LANES

    def each(act):
        for origin in range(n):

            @pl.when(jnp.logical_and(core == 0, me != origin))
            def _(origin=origin):
                rows = pl.ds((origin + 1) * block - tail, tail)
                act(pltpu.make_async_copy(pieces.at[origin], out.at[rows], sem.at[origin]))

    each(lambda copy: copy.start())
    each(lambda copy: copy.wait())


def on_device(n, cores, *args):
    weights, (norm_train, norm_step) = list(args[:12]), args[12:]
    bases = weights[0::3]
    (size,) = norm_train.shape
    sizes = [size, *(size for w in bases for size in w.shape)]
    if cores != 2 or any(size % LANES for size in sizes):
        return plain(*args)
    rows = size // LANES
    shapes = [(w.shape[1], w.shape[0] * n) for w in bases[:3]]
    shapes.append((bases[3].shape[1] * n, bases[3].shape[0]))
    slots = sum(w.shape[1] // LANES for w in bases) + 1
    in_hbm = pl.BlockSpec(memory_space=pltpu.HBM)
    in_vmem = pl.BlockSpec(memory_space=pltpu.VMEM)
    weights[1::3] = [low.T for low in weights[1::3]]
    norms = [norm_train.reshape(rows, LANES), norm_step.reshape(rows, LANES)]
    given = [pltpu.with_memory_space_constraint(array, pltpu.HBM) for array in weights + norms]
    gathered = pl.pallas_call(
        functools.partial(body, n),
        out_shape=[pltpu.VMEM(shape, jnp.bfloat16) for shape in shapes]
        + [pltpu.VMEM((n, cores, rows, LANES), jnp.float32)],
        in_specs=[in_hbm] * 14,
        out_specs=[in_vmem] * 5,
        scratch_shapes=[pltpu.VMEM(array.shape, array.dtype) for array in given]
        + [
            pltpu.SemaphoreType.DMA((15,)),
            pltpu.SemaphoreType.DMA((n, slots)),
            pltpu.SemaphoreType.DMA((slots,)),
            pltpu.SemaphoreType.DMA((n, slots)),
            pltpu.SemaphoreType.DMA((2,)),
        ],
        compiler_params=pltpu.CompilerParams(
            collective_id=0, has_side_effects=True, vmem_limit_bytes=40 * 2**20
        ),
        name="merge_gather",
    )(*given)
    norm_rows = n * cores * rows
    *finals, norm = pl.pallas_call(
        functools.partial(store, n, cores),
        out_shape=[jax.ShapeDtypeStruct(shape, jnp.bfloat16) for shape in shapes]
        + [jax.ShapeDtypeStruct((norm_rows, LANES), jnp.bfloat16)],
        in_specs=[in_vmem] * 5,
        out_specs=[in_hbm] * 4 + [in_vmem],
        scratch_shapes=[
            pltpu.VMEM((norm_rows, LANES), jnp.float32),
            pltpu.SemaphoreType.DMA((sum(-(-shape[0] // COPY_ROWS) for shape in shapes[:3]),)),
            pltpu.SemaphoreType.DMA((n, 2)),
        ],
        compiler_params=pltpu.CompilerParams(vmem_limit_bytes=20 * 2**20),
        name="store",
    )(*gathered)
    columns = shapes[3][1]
    tail = late_pieces(bases[3].shape[1]) * LANES
    pieces = pl.pallas_call(
        functools.partial(late, n),
        out_shape=pltpu.VMEM((n, tail, columns), jnp.bfloat16),
        in_specs=[in_vmem, in_hbm],
        out_specs=in_vmem,
        scratch_shapes=[
            pltpu.SemaphoreType.DMA((n, LATE_STEPS)),
            pltpu.SemaphoreType.DMA((LATE_STEPS,)),
            pltpu.SemaphoreType.DMA((n, LATE_STEPS)),
        ],
        compiler_params=pltpu.CompilerParams(
            collective_id=1, has_side_effects=True, vmem_limit_bytes=20 * 2**20
        ),
        name="late",
    )(gathered[3], pltpu.with_memory_space_constraint(finals[3], pltpu.HBM))
    finals[3] = pl.pallas_call(
        functools.partial(store_late, n),
        out_shape=jax.ShapeDtypeStruct(shapes[3], jnp.bfloat16),
        in_specs=[in_vmem, in_hbm],
        out_specs=in_hbm,
        input_output_aliases={1: 0},
        scratch_shapes=[pltpu.SemaphoreType.DMA((n,))],
        compiler_params=pltpu.CompilerParams(vmem_limit_bytes=20 * 2**20),
        name="store_late",
    )(pieces, finals[3])
    return (*finals, norm.reshape(-1))


def solution(mesh):
    placed = (
        P(("shift", "shard"), "width"),
        P(("shift", "shard"), None),
        P("shift", "width"),
        P(("shift", "shard"), "width"),
        P(("shift", "shard"), None),
        P("shift", "width"),
        P(("shift", "shard"), "width"),
        P(("shift", "shard"), None),
        P("shift", "width"),
        P(("shift", "width"), "shard"),
        P(("shift", "width"), None),
        P("shift", "shard"),
        P(("shift", "shard", "width")),
        P(("shift", "shard", "width")),
    )
    return jax.shard_map(
        functools.partial(on_device, mesh.shape["shard"], mesh.shape["width"]),
        mesh=mesh,
        in_specs=placed,
        out_specs=(
            P(("shift", "width"), None),
            P(("shift", "width"), None),
            P(("shift", "width"), None),
            P("shift", "width"),
            P("shift"),
        ),
        check_vma=False,
    )
```
